32 devices in a mesh: kx: 8 (over z, x), cz: 4 (over y, core).
Axes of the slice: x: 2, y: 2, z: 4, core: 2. Of those that a mesh axis runs over, the one named last changes fastest.
Arguments:
- field_modes: bfloat16 [512, 4, 12288], P('cz', None, 'kx'), may hold values from -6 to 6
- cotangent: bfloat16 [512, 4, 12288], P('cz', None, 'kx'), may hold values from -6 to 6
Outputs:
- mode_gradient: bfloat16 [512, 4, 12288], P('cz', None, 'kx')
The draws below stay inside these ranges and needn't reach their ends.
All inputs are finite; a program needn't handle non-finite values.
Results may differ from the reference program's by a relative error of at most 0.009.
Values may be sent and summed in bfloat16 or wider, within the bound.
No kernel may reach another device: no remote copies, remote signals or barrier semaphores. Data moves between devices by JAX's collectives and lax.ppermute only.
A program may use at most 128 MiB of HBM per device.

```python
import math
import jax
import jax.numpy as jnp
from jax import lax

FIELDS = 4
NZ = 512
MZ = 768
NX = 768
Y = 16


def steps_of(key, dims, pieces, smallest, largest):
    gain, own = 1.0, jax.random.fold_in(key, 6)
    for axis_at, shards_of in pieces:
        heights = jnp.exp(jax.random.uniform(jax.random.fold_in(own, axis_at), (shards_of,), jnp.float32, smallest / len(pieces), largest / len(pieces)))
        gain = gain * jnp.repeat(heights, dims[axis_at] // shards_of).reshape([-1 if axis == axis_at else 1 for axis in range(len(dims))])
    return gain


def normal_values(rng, shape, spread, bound, cuts=(), kind=jnp.bfloat16):
    factor_of = steps_of(rng, shape, cuts, -0.22, 0.18) if cuts else 1.0
    drawn = jax.random.normal(rng, shape, jnp.float32) * spread * factor_of
    return jnp.minimum(jnp.maximum(drawn, -bound), bound).astype(kind)


def setup_inputs(seed: int = 0) -> dict:
    key_of = jax.random.split(jax.random.key(seed), 3)
    return {
        "field_modes": normal_values(key_of[0], (NZ, FIELDS, NX * Y), 1.0, 6.0, ((0, 4), (2, 8))),
        "cotangent": normal_values(key_of[1], (NZ, FIELDS, NX * Y), 1.0, 6.0, ((0, 4), (2, 8))),
    }


def cosine_table():
    row_index = jnp.arange(MZ, dtype=jnp.int32)
    col_index = jnp.arange(NZ, dtype=jnp.int32)
    position = col_index[None, :] * (2 * row_index[:, None] + 1) % (4 * MZ)
    return jnp.cos(jnp.pi * position.astype(jnp.float32) / (2 * MZ))

def hartley_table():
    points = jnp.arange(NX, dtype=jnp.int32)
    position = points[:, None] * points[None, :] % NX
    phases = 2.0 * jnp.pi * position.astype(jnp.float32) / NX
    return ((jnp.cos(phases) + jnp.sin(phases)) / math.sqrt(NX)).astype(jnp.bfloat16)

def product_gradient(fields, adjoint):
    vertical = fields[2]
    return jnp.stack([adjoint[0] * vertical, adjoint[1] * vertical, adjoint[0] * fields[0] + adjoint[1] * fields[1] + 2.0 * adjoint[2] * vertical + adjoint[3] * fields[3], adjoint[3] * vertical]).astype(jnp.bfloat16)

def reference(field_modes, cotangent):
    highest = lax.Precision.HIGHEST
    field_grid = field_modes.reshape(NZ, FIELDS, NX, Y)
    cotangent_grid = cotangent.reshape(NZ, FIELDS, NX, Y)
    cosines = cosine_table()
    synthesis_full = (cosines * math.sqrt(2.0 / NZ)).astype(jnp.bfloat16).astype(jnp.float32)
    projection_full = (cosines * math.sqrt(2.0 / MZ)).astype(jnp.bfloat16).astype(jnp.float32)
    hartley_full = hartley_table().astype(jnp.float32)
    block_rows = 8
    block_count = Y // block_rows

    def one_block(position):
        first_row = position * block_rows
        mode_block = lax.dynamic_slice_in_dim(field_grid, first_row, block_rows, 3).astype(jnp.float32)
        adjoint_block = lax.dynamic_slice_in_dim(cotangent_grid, first_row, block_rows, 3).astype(jnp.float32)
        lifted_fields = jnp.einsum('zk,kfmy->fzmy', synthesis_full, mode_block, precision=highest).astype(jnp.bfloat16).astype(jnp.float32)
        lifted_adjoint = jnp.einsum('zk,kfmy->fzmy', projection_full, adjoint_block, precision=highest).astype(jnp.bfloat16).astype(jnp.float32)
        fields = jnp.einsum('xm,fzmy->fzxy', hartley_full, lifted_fields, precision=highest)
        adjoint = jnp.einsum('xm,fzmy->fzxy', hartley_full, lifted_adjoint, precision=highest)
        gradient = product_gradient(fields, adjoint).astype(jnp.float32)
        turned = jnp.einsum('xm,fzxy->fzmy', hartley_full, gradient, precision=highest).astype(jnp.bfloat16).astype(jnp.float32)
        spectral = jnp.einsum('zk,fzmy->kfmy', synthesis_full, turned, precision=highest)
        return spectral.astype(jnp.bfloat16)
    blocks = lax.map(one_block, jnp.arange(block_count, dtype=jnp.int32))
    return jnp.moveaxis(blocks, 0, 3).reshape(NZ, FIELDS, NX * Y)
```

```python
import functools
import math

import jax
import jax.numpy as jnp
import numpy as np
from jax import lax
from jax.experimental import pallas as pl
from jax.experimental.pallas import tpu as pltpu
from jax.sharding import PartitionSpec as P

NZ = 512
MZ = 768
NX = 768
Y = 16

BF16 = jnp.bfloat16
F32 = jnp.float32

INBOUND = (((0, 2), (1, 0), (1, 1), (1, 3)), ((0, 0), (0, 1), (0, 3), (1, 2)))
OUTBOUND = ((0, 1, 3), (2,))


def cosine_table():
    row_index = jnp.arange(MZ, dtype=jnp.int32)
    col_index = jnp.arange(NZ, dtype=jnp.int32)
    position = col_index[None, :] * (2 * row_index[:, None] + 1) % (4 * MZ)
    return jnp.cos(jnp.pi * position.astype(jnp.float32) / (2 * MZ))


def hartley_table():
    points = jnp.arange(NX, dtype=jnp.int32)
    position = points[:, None] * points[None, :] % NX
    phases = 2.0 * jnp.pi * position.astype(jnp.float32) / NX
    return ((jnp.cos(phases) + jnp.sin(phases)) / math.sqrt(NX)).astype(jnp.bfloat16)


def product_gradient(fields, adjoint):
    vertical = fields[2]
    return jnp.stack(
        [
            adjoint[0] * vertical,
            adjoint[1] * vertical,
            adjoint[0] * fields[0]
            + adjoint[1] * fields[1]
            + 2.0 * adjoint[2] * vertical
            + adjoint[3] * fields[3],
            adjoint[3] * vertical,
        ]
    ).astype(jnp.bfloat16)


def general_on_device(field_modes, cotangent):
    local_modes = field_modes.shape[0]
    field_count = field_modes.shape[1]
    local_columns = field_modes.shape[2] // Y
    field_grid = field_modes.reshape(local_modes, field_count, local_columns, Y)
    cotangent_grid = cotangent.reshape(local_modes, field_count, local_columns, Y)
    cosines = cosine_table()
    synthesis = (cosines * math.sqrt(2.0 / NZ)).astype(jnp.bfloat16)
    projection = (cosines * math.sqrt(2.0 / MZ)).astype(jnp.bfloat16)
    hartley = hartley_table()
    lifted = jnp.concatenate(
        [
            jnp.einsum(
                "zk,kfxy->yfxz",
                synthesis,
                lax.all_to_all(field_grid, "cz", split_axis=3, concat_axis=0, tiled=True),
                preferred_element_type=jnp.float32,
            ).astype(jnp.bfloat16),
            jnp.einsum(
                "zk,kfxy->yfxz",
                projection,
                lax.all_to_all(cotangent_grid, "cz", split_axis=3, concat_axis=0, tiled=True),
                preferred_element_type=jnp.float32,
            ).astype(jnp.bfloat16),
        ],
        axis=1,
    )
    piece = lax.all_to_all(lifted, "kx", split_axis=3, concat_axis=2, tiled=True)
    fields = jnp.einsum(
        "xm,yfmz->fyzx", hartley, piece[:, :field_count], preferred_element_type=jnp.float32
    )
    adjoint = jnp.einsum(
        "xm,yfmz->fyzx", hartley, piece[:, field_count:], preferred_element_type=jnp.float32
    )
    gradient = product_gradient(fields, adjoint)
    turned = jnp.einsum(
        "xm,fyzx->yfmz", hartley, gradient, preferred_element_type=jnp.float32
    ).astype(jnp.bfloat16)
    returned = lax.all_to_all(turned, "kx", split_axis=2, concat_axis=3, tiled=True)
    spectral = jnp.einsum(
        "zk,yfxz->kfxy", synthesis, returned, preferred_element_type=jnp.float32
    ).astype(jnp.bfloat16)
    result = lax.all_to_all(spectral, "cz", split_axis=0, concat_axis=3, tiled=True)
    return result.reshape(local_modes, field_count, local_columns * Y)


class Plan:
    def __init__(self, kx_size, cz_size, shape):
        self.kx = kx_size
        self.cz = cz_size
        self.modes, self.fields, columns = shape
        self.columns = columns // Y
        self.turns = max(Y // kx_size, 1)
        self.cores = cz_size // self.turns
        self.rows = kx_size * self.turns
        self.group = 256 // Y
        self.points = NX // self.cores
        self.depth = self.turns * self.modes

    @property
    def fits(self):
        return (
            self.rows == Y
            and self.rows & (self.rows - 1) == 0
            and self.turns * self.cores == self.cz
            and self.cores == 2
            and self.modes % 128 == 0
            and self.columns % self.group == 0
            and self.points % 128 == 0
        )

    @property
    def order(self):
        top = self.rows // 2
        far = [s ^ t for s in (top, top + top // 2) for t in range(self.rows // 4)]
        near = [s ^ t for s in (top // 2, 0) for t in range(self.rows // 4)]
        first = [s for pair in zip(far[: len(far) // 2], far[len(far) // 2 :]) for s in pair]
        return first + [s for s in near if s] + [0]

    def across(self, step):
        pairs = []
        for kx in range(self.kx):
            for cz in range(self.cz):
                ca, cb = divmod(cz, self.cores)
                other = (kx * self.turns + ca) ^ step
                target = other // self.turns * self.cz + other % self.turns * self.cores + cb
                pairs.append((kx * self.cz + cz, target))
        return pairs

    def core_swap(self):
        return [(d, d ^ 1) for d in range(self.kx * self.cz)]


def row_index(plan):
    return lax.axis_index("kx") * plan.turns + lax.axis_index("cz") // plan.cores


def core_index(plan):
    return lax.rem(lax.axis_index("cz"), plan.cores)


def matmul(a, b, dims):
    return lax.dot_general(a, b, (dims, ((), ())), preferred_element_type=F32)


def pack_kernel(plan, items, *refs):
    arrays, (turn_ref, *out_refs), (wide, packed) = refs[:2], refs[2:-2], refs[-2:]
    fields = plan.fields
    arrays_used = sorted({array for array, _ in items})
    tiles = plan.columns * Y // 128
    for array in arrays_used:
        for k in range(plan.modes):
            for tile in range(tiles):
                wide[tile, pl.ds(k * fields, fields), :] = arrays[array][
                    k, :, tile * 128 : (tile + 1) * 128
                ].astype(F32)
        for place, (owner, field) in enumerate(items):
            if owner != array:
                continue
            for block in range(plan.columns // plan.group):
                rows = jnp.concatenate(
                    [
                        wide[tile, pl.ds(field, plan.modes, stride=fields), :].astype(BF16)
                        for tile in (2 * block, 2 * block + 1)
                    ],
                    axis=1,
                )
                turned = matmul(turn_ref[...], rows, ((1,), (1,))).astype(BF16)
                packed[
                    :,
                    block * plan.group : (block + 1) * plan.group,
                    place * plan.modes : (place + 1) * plan.modes,
                ] = turned.reshape(Y, plan.group, plan.modes)
    me = row_index(plan)
    for step, out_ref in zip(plan.order, out_refs):
        out_ref[...] = packed[me ^ step]


def hartley_kernel(plan, count, *refs):
    hartley_ref, pieces = refs[0], refs[1 : 1 + plan.rows]
    own_ref, send_ref, gathered = refs[1 + plan.rows :]
    me, core = row_index(plan), core_index(plan)
    for step, piece in zip(plan.order, pieces):
        other = me ^ step
        at = pl.multiple_of(other // plan.turns * plan.columns, 16)
        gathered[other % plan.turns, pl.ds(at, plan.columns), :] = piece[...]
    for half, out_ref in ((core, own_ref), (1 - core, send_ref)):
        table = hartley_ref[pl.ds(pl.multiple_of(half * plan.points, 128), plan.points), :]
        for turn in range(plan.turns):
            result = matmul(table, gathered[turn], ((1,), (0,))).astype(BF16)
            for item in range(count):
                at = item * plan.depth + turn * plan.modes
                out_ref[:, at : at + plan.modes] = result[
                    :, item * plan.modes : (item + 1) * plan.modes
                ]


def lift(plan, table, own_ref, recv_ref, rows, item):
    core = core_index(plan)
    at = pl.ds(item * plan.depth, plan.depth)
    return matmul(own_ref[rows, at], table[core], ((1,), (0,))) + matmul(
        recv_ref[rows, at], table[1 - core], ((1,), (0,))
    )


def lower(plan, table, value, out_refs, rows, item):
    core = core_index(plan)
    at = pl.ds(item * plan.depth, plan.depth)
    for half, out_ref in zip((core, 1 - core), out_refs):
        out_ref[rows, at] = matmul(value, table[half], ((1,), (1,))).astype(BF16)


TILE = 128


def first_kernel(plan, synthesis, projection, own, recv, own_out, send_out, kept):
    def body(tile, _):
        rows = pl.ds(pl.multiple_of(tile * TILE, TILE), TILE)
        vertical = lift(plan, synthesis, own, recv, rows, 0)
        kept[0, rows, :] = vertical
        for item in range(1, 4):
            adjoint = lift(plan, projection, own, recv, rows, item)
            kept[item, rows, :] = adjoint
            lower(
                plan, synthesis, (adjoint * vertical).astype(BF16), (own_out, send_out), rows, item - 1
            )
        return 0

    lax.fori_loop(0, plan.points // TILE, body, 0)


def second_kernel(plan, synthesis, projection, own, recv, kept, own_out, send_out):
    def body(tile, _):
        rows = pl.ds(pl.multiple_of(tile * TILE, TILE), TILE)
        total = kept[1, rows, :] * lift(plan, synthesis, own, recv, rows, 0)
        total += kept[2, rows, :] * lift(plan, synthesis, own, recv, rows, 1)
        total += 2.0 * lift(plan, projection, own, recv, rows, 3) * kept[0, rows, :]
        total += kept[3, rows, :] * lift(plan, synthesis, own, recv, rows, 2)
        lower(plan, synthesis, total.astype(BF16), (own_out, send_out), rows, 0)
        return 0

    lax.fori_loop(0, plan.points // TILE, body, 0)


def inverse_kernel(plan, count, *refs):
    hartley_ref, own_ref, recv_ref = refs[:3]
    out_refs, turned = refs[3:-1], refs[-1]
    me, core = row_index(plan), core_index(plan)
    halves = [
        hartley_ref[:, pl.ds(pl.multiple_of(half * plan.points, 128), plan.points)]
        for half in (core, 1 - core)
    ]
    for item in range(count):
        at = slice(item * plan.depth, (item + 1) * plan.depth)
        result = matmul(halves[0], own_ref[:, at], ((1,), (0,))) + matmul(
            halves[1], recv_ref[:, at], ((1,), (0,))
        )
        result = result.astype(BF16)
        for turn in range(plan.turns):
            turned[turn, :, item * plan.modes : (item + 1) * plan.modes] = result[
                :, turn * plan.modes : (turn + 1) * plan.modes
            ]
    for step, out_ref in zip(plan.order, out_refs):
        other = me ^ step
        at = pl.multiple_of(other // plan.turns * plan.columns, 16)
        out_ref[...] = turned[other % plan.turns, pl.ds(at, plan.columns), :]


def unpack_kernel(plan, *refs):
    turn_ref = refs[0]
    groups = [refs[1 + g * plan.rows : 1 + (g + 1) * plan.rows] for g in range(len(OUTBOUND))]
    out_ref, wide, gathered = refs[-3:]
    me = row_index(plan)
    fields = plan.fields
    for group, pieces in zip(OUTBOUND, groups):
        for step, piece in zip(plan.order, pieces):
            for item, field in enumerate(group):
                gathered[field, me ^ step] = piece[:, item * plan.modes : (item + 1) * plan.modes]
    for field in range(fields):
        for block in range(plan.columns // plan.group):
            rows = gathered[field, :, block * plan.group : (block + 1) * plan.group, :]
            rows = rows.reshape(256, plan.modes)
            result = matmul(rows, turn_ref[...], ((0,), (0,)))
            for side in range(2):
                wide[2 * block + side, pl.ds(field, plan.modes, stride=fields), :] = result[
                    :, side * 128 : (side + 1) * 128
                ]
    for k in range(plan.modes):
        for tile in range(plan.columns * Y // 128):
            out_ref[k, :, tile * 128 : (tile + 1) * 128] = wide[
                tile, pl.ds(k * fields, fields), :
            ].astype(BF16)


def call(kernel, outs, scratch, flops, moved, name, *args):
    space = pl.BlockSpec(memory_space=pltpu.VMEM)
    single = not isinstance(outs, (list, tuple))
    return pl.pallas_call(
        kernel,
        out_shape=outs,
        in_specs=[space] * len(args),
        out_specs=space if single else [space] * len(outs),
        scratch_shapes=scratch,
        cost_estimate=pl.CostEstimate(flops=flops, bytes_accessed=moved, transcendentals=0),
        name=name,
    )(*args)


def tables(plan):
    z, k = np.arange(MZ), np.arange(NZ)
    cosines = np.cos(np.pi * (k[:, None] * (2 * z[None, :] + 1) % (4 * MZ)) / (2 * MZ))
    cosines = cosines.reshape(plan.turns, plan.cores, plan.modes, MZ).swapaxes(0, 1)
    cosines = cosines.reshape(plan.cores, plan.depth, MZ).astype(np.float32)
    points = np.arange(NX)
    phases = 2.0 * np.pi * (points[:, None] * points[None, :] % NX) / NX
    hartley = ((np.cos(phases) + np.sin(phases)) / math.sqrt(NX)).astype(np.float32)
    turn = np.zeros((Y, plan.group, plan.group, Y), np.float32)
    for y in range(Y):
        for m in range(plan.group):
            turn[y, m, m, y] = 1.0
    return (
        jnp.asarray((cosines * np.float32(math.sqrt(2.0 / NZ))).astype(BF16)),
        jnp.asarray((cosines * np.float32(math.sqrt(2.0 / MZ))).astype(BF16)),
        jnp.asarray(hartley.astype(BF16)),
        jnp.asarray(turn.reshape(256, 256).astype(BF16)),
    )


def exchange(plan, pieces):
    return [
        lax.ppermute(piece, ("kx", "cz"), plan.across(step)) if step else piece
        for step, piece in zip(plan.order, pieces)
    ]


def row_on_device(plan, field_modes, cotangent):
    synthesis, projection, hartley, turn = tables(plan)
    shape = jax.ShapeDtypeStruct
    local = field_modes.size
    arrived = []
    for number, items in enumerate(INBOUND):
        width = len(items) * plan.modes
        pieces = call(
            functools.partial(pack_kernel, plan, items),
            [shape((plan.columns, width), BF16)] * plan.rows,
            [
                pltpu.VMEM((plan.columns * Y // 128, plan.fields * plan.modes, 128), F32),
                pltpu.VMEM((plan.rows, plan.columns, width), BF16),
            ],
            2 * 256 * local // plan.fields * len(items),
            4 * local,
            f"pack{number}",
            field_modes,
            cotangent,
            turn,
        )
        arrived.append(exchange(plan, pieces))

    def swap(value):
        return lax.ppermute(value, ("kx", "cz"), plan.core_swap())

    returned = []
    kept = None
    for number, (items, outputs) in enumerate(zip(INBOUND, OUTBOUND)):
        count = len(items)
        width = count * plan.modes
        wide = count * plan.depth
        own, send = call(
            functools.partial(hartley_kernel, plan, count),
            [shape((plan.points, wide), BF16)] * 2,
            [pltpu.VMEM((plan.turns, NX, width), BF16)],
            2 * NX * NX * plan.turns * width,
            4 * NX * plan.turns * width,
            f"hartley{number}",
            hartley,
            *arrived[number],
        )
        recv = swap(send)
        out_wide = len(outputs) * plan.depth
        outs = [shape((plan.points, out_wide), BF16)] * 2
        flops = 2 * plan.points * NZ * MZ * (count + len(outputs))
        if number == 0:
            own, send, kept = call(
                functools.partial(first_kernel, plan),
                outs + [shape((count, plan.points, MZ), F32)],
                [],
                flops,
                4 * count * plan.points * MZ,
                "fluxes",
                synthesis,
                projection,
                own,
                recv,
            )
        else:
            own, send = call(
                functools.partial(second_kernel, plan),
                outs,
                [],
                flops,
                4 * count * plan.points * MZ,
                "vertical",
                synthesis,
                projection,
                own,
                recv,
                kept,
            )
        recv = swap(send)
        pieces = call(
            functools.partial(inverse_kernel, plan, len(outputs)),
            [shape((plan.columns, len(outputs) * plan.modes), BF16)] * plan.rows,
            [pltpu.VMEM((plan.turns, NX, len(outputs) * plan.modes), BF16)],
            2 * NX * NX * out_wide,
            4 * NX * out_wide,
            f"inverse{number}",
            hartley,
            own,
            recv,
        )
        returned += exchange(plan, pieces)
    return call(
        functools.partial(unpack_kernel, plan),
        shape(field_modes.shape, BF16),
        [
            pltpu.VMEM((plan.columns * Y // 128, plan.fields * plan.modes, 128), F32),
            pltpu.VMEM((plan.fields, plan.rows, plan.columns, plan.modes), BF16),
        ],
        2 * 256 * local,
        4 * local,
        "unpack",
        turn,
        *returned,
    )


def on_device(kx_size, cz_size, field_modes, cotangent):
    plan = Plan(kx_size, cz_size, field_modes.shape)
    if plan.fits:
        return row_on_device(plan, field_modes, cotangent)
    return general_on_device(field_modes, cotangent)


def solution(mesh):
    return jax.shard_map(
        functools.partial(on_device, mesh.shape["kx"], mesh.shape["cz"]),
        mesh=mesh,
        in_specs=(P("cz", None, "kx"), P("cz", None, "kx")),
        out_specs=P("cz", None, "kx"),
        check_vma=False,
    )
```

```python
import functools
import math

import jax
import jax.numpy as jnp
import numpy as np
from jax import lax
from jax.experimental import pallas as pl
from jax.experimental.pallas import tpu as pltpu
from jax.sharding import PartitionSpec as P


NZ = 512
MZ = 768
NX = 768
Y = 16

BF16 = jnp.bfloat16
F32 = jnp.float32

INBOUND = (((0, 2), (1, 0), (1, 1), (1, 3)), ((0, 0), (0, 1), (0, 3), (1, 2)))
OUTBOUND = ((0, 1, 3), (2,))


def cosine_table():
    row_index = jnp.arange(MZ, dtype=jnp.int32)
    col_index = jnp.arange(NZ, dtype=jnp.int32)
    position = col_index[None, :] * (2 * row_index[:, None] + 1) % (4 * MZ)
    return jnp.cos(jnp.pi * position.astype(jnp.float32) / (2 * MZ))


def hartley_table():
    points = jnp.arange(NX, dtype=jnp.int32)
    position = points[:, None] * points[None, :] % NX
    phases = 2.0 * jnp.pi * position.astype(jnp.float32) / NX
    return ((jnp.cos(phases) + jnp.sin(phases)) / math.sqrt(NX)).astype(jnp.bfloat16)


def product_gradient(fields, adjoint):
    vertical = fields[2]
    return jnp.stack(
        [
            adjoint[0] * vertical,
            adjoint[1] * vertical,
            adjoint[0] * fields[0]
            + adjoint[1] * fields[1]
            + 2.0 * adjoint[2] * vertical
            + adjoint[3] * fields[3],
            adjoint[3] * vertical,
        ]
    ).astype(jnp.bfloat16)


def general_on_device(field_modes, cotangent):
    local_modes = field_modes.shape[0]
    field_count = field_modes.shape[1]
    local_columns = field_modes.shape[2] // Y
    field_grid = field_modes.reshape(local_modes, field_count, local_columns, Y)
    cotangent_grid = cotangent.reshape(local_modes, field_count, local_columns, Y)
    cosines = cosine_table()
    synthesis = (cosines * math.sqrt(2.0 / NZ)).astype(jnp.bfloat16)
    projection = (cosines * math.sqrt(2.0 / MZ)).astype(jnp.bfloat16)
    hartley = hartley_table()
    lifted = jnp.concatenate(
        [
            jnp.einsum(
                "zk,kfxy->yfxz",
                synthesis,
                lax.all_to_all(field_grid, "cz", split_axis=3, concat_axis=0, tiled=True),
                preferred_element_type=jnp.float32,
            ).astype(jnp.bfloat16),
            jnp.einsum(
                "zk,kfxy->yfxz",
                projection,
                lax.all_to_all(cotangent_grid, "cz", split_axis=3, concat_axis=0, tiled=True),
                preferred_element_type=jnp.float32,
            ).astype(jnp.bfloat16),
        ],
        axis=1,
    )
    piece = lax.all_to_all(lifted, "kx", split_axis=3, concat_axis=2, tiled=True)
    fields = jnp.einsum(
        "xm,yfmz->fyzx", hartley, piece[:, :field_count], preferred_element_type=jnp.float32
    )
    adjoint = jnp.einsum(
        "xm,yfmz->fyzx", hartley, piece[:, field_count:], preferred_element_type=jnp.float32
    )
    gradient = product_gradient(fields, adjoint)
    turned = jnp.einsum(
        "xm,fyzx->yfmz", hartley, gradient, preferred_element_type=jnp.float32
    ).astype(jnp.bfloat16)
    returned = lax.all_to_all(turned, "kx", split_axis=2, concat_axis=3, tiled=True)
    spectral = jnp.einsum(
        "zk,yfxz->kfxy", synthesis, returned, preferred_element_type=jnp.float32
    ).astype(jnp.bfloat16)
    result = lax.all_to_all(spectral, "cz", split_axis=0, concat_axis=3, tiled=True)
    return result.reshape(local_modes, field_count, local_columns * Y)


class Plan:
    def __init__(self, kx_size, cz_size, shape):
        self.kx = kx_size
        self.cz = cz_size
        self.modes, self.fields, columns = shape
        self.columns = columns // Y
        self.turns = max(Y // kx_size, 1)
        self.cores = cz_size // self.turns
        self.rows = kx_size * self.turns
        self.group = 256 // Y
        self.points = NX // self.cores
        self.depth = self.turns * self.modes

    @property
    def fits(self):
        return (
            self.rows == Y
            and self.rows & (self.rows - 1) == 0
            and self.turns * self.cores == self.cz
            and self.cores == 2
            and self.modes % 128 == 0
            and self.columns % self.group == 0
            and self.points % 128 == 0
        )

    @property
    def order(self):
        top = self.rows // 2
        far = [s ^ t for s in (top, top + top // 2) for t in range(self.rows // 4)]
        near = [s ^ t for s in (top // 2, 0) for t in range(self.rows // 4)]
        first = [s for pair in zip(far[: len(far) // 2], far[len(far) // 2 :]) for s in pair]
        return first + [s for s in near if s] + [0]

    def across(self, step):
        pairs = []
        for kx in range(self.kx):
            for cz in range(self.cz):
                ca, cb = divmod(cz, self.cores)
                other = (kx * self.turns + ca) ^ step
                target = other // self.turns * self.cz + other % self.turns * self.cores + cb
                pairs.append((kx * self.cz + cz, target))
        return pairs

    def core_swap(self):
        return [(d, d ^ 1) for d in range(self.kx * self.cz)]


def row_index(plan):
    return lax.axis_index("kx") * plan.turns + lax.axis_index("cz") // plan.cores


def core_index(plan):
    return lax.rem(lax.axis_index("cz"), plan.cores)


def matmul(a, b, dims):
    return lax.dot_general(a, b, (dims, ((), ())), preferred_element_type=F32)


def pack_kernel(plan, items, *refs):
    arrays, (turn_ref, *out_refs), (wide, packed) = refs[:2], refs[2:-2], refs[-2:]
    fields = plan.fields
    arrays_used = sorted({array for array, _ in items})
    tiles = plan.columns * Y // 128
    for array in arrays_used:
        for k in range(plan.modes):
            for tile in range(tiles):
                wide[tile, pl.ds(k * fields, fields), :] = arrays[array][
                    k, :, tile * 128 : (tile + 1) * 128
                ].astype(F32)
        for place, (owner, field) in enumerate(items):
            if owner != array:
                continue
            for block in range(plan.columns // plan.group):
                rows = jnp.concatenate(
                    [
                        wide[tile, pl.ds(field, plan.modes, stride=fields), :].astype(BF16)
                        for tile in (2 * block, 2 * block + 1)
                    ],
                    axis=1,
                )
                turned = matmul(turn_ref[...], rows, ((1,), (1,))).astype(BF16)
                packed[
                    :,
                    block * plan.group : (block + 1) * plan.group,
                    place * plan.modes : (place + 1) * plan.modes,
                ] = turned.reshape(Y, plan.group, plan.modes)
    me = row_index(plan)
    for step, out_ref in zip(plan.order, out_refs):
        out_ref[...] = packed[me ^ step]


def hartley_kernel(plan, count, *refs):
    hartley_ref, pieces = refs[0], refs[1 : 1 + plan.rows]
    own_ref, send_ref, gathered = refs[1 + plan.rows :]
    me, core = row_index(plan), core_index(plan)
    for step, piece in zip(plan.order, pieces):
        other = me ^ step
        at = pl.multiple_of(other // plan.turns * plan.columns, 16)
        gathered[other % plan.turns, pl.ds(at, plan.columns), :] = piece[...]
    for half, out_ref in ((core, own_ref), (1 - core, send_ref)):
        table = hartley_ref[pl.ds(pl.multiple_of(half * plan.points, 128), plan.points), :]
        for turn in range(plan.turns):
            result = matmul(table, gathered[turn], ((1,), (0,))).astype(BF16)
            for item in range(count):
                at = item * plan.depth + turn * plan.modes
                out_ref[:, at : at + plan.modes] = result[
                    :, item * plan.modes : (item + 1) * plan.modes
                ]


def lift(plan, table, own_ref, recv_ref, rows, item):
    core = core_index(plan)
    at = pl.ds(item * plan.depth, plan.depth)
    return matmul(own_ref[rows, at], table[core], ((1,), (0,))) + matmul(
        recv_ref[rows, at], table[1 - core], ((1,), (0,))
    )


def lower(plan, table, value, out_refs, rows, item):
    core = core_index(plan)
    at = pl.ds(item * plan.depth, plan.depth)
    for half, out_ref in zip((core, 1 - core), out_refs):
        out_ref[rows, at] = matmul(value, table[half], ((1,), (1,))).astype(BF16)


TILE = 128
KERNEL_VMEM = 24 * 1024 * 1024


def first_kernel(plan, synthesis, projection, own, recv, own_out, send_out, kept):
    def body(tile, _):
        rows = pl.ds(pl.multiple_of(tile * TILE, TILE), TILE)
        vertical = lift(plan, synthesis, own, recv, rows, 0)
        kept[0, rows, :] = vertical
        for item in range(1, 4):
            adjoint = lift(plan, projection, own, recv, rows, item)
            kept[item, rows, :] = adjoint
            lower(
                plan, synthesis, (adjoint * vertical).astype(BF16), (own_out, send_out), rows, item - 1
            )
        return 0

    lax.fori_loop(0, plan.points // TILE, body, 0)


def second_kernel(plan, synthesis, projection, own, recv, kept, own_out, send_out):
    def body(tile, _):
        rows = pl.ds(pl.multiple_of(tile * TILE, TILE), TILE)
        total = kept[1, rows, :] * lift(plan, synthesis, own, recv, rows, 0)
        total += kept[2, rows, :] * lift(plan, synthesis, own, recv, rows, 1)
        total += 2.0 * lift(plan, projection, own, recv, rows, 3) * kept[0, rows, :]
        total += kept[3, rows, :] * lift(plan, synthesis, own, recv, rows, 2)
        lower(plan, synthesis, total.astype(BF16), (own_out, send_out), rows, 0)
        return 0

    lax.fori_loop(0, plan.points // TILE, body, 0)


def inverse_kernel(plan, count, *refs):
    hartley_ref, own_ref, recv_ref = refs[:3]
    out_refs, turned = refs[3:-1], refs[-1]
    me, core = row_index(plan), core_index(plan)
    halves = [
        hartley_ref[:, pl.ds(pl.multiple_of(half * plan.points, 128), plan.points)]
        for half in (core, 1 - core)
    ]
    for item in range(count):
        at = slice(item * plan.depth, (item + 1) * plan.depth)
        result = matmul(halves[0], own_ref[:, at], ((1,), (0,))) + matmul(
            halves[1], recv_ref[:, at], ((1,), (0,))
        )
        result = result.astype(BF16)
        for turn in range(plan.turns):
            turned[turn, :, item * plan.modes : (item + 1) * plan.modes] = result[
                :, turn * plan.modes : (turn + 1) * plan.modes
            ]
    for step, out_ref in zip(plan.order, out_refs):
        other = me ^ step
        at = pl.multiple_of(other // plan.turns * plan.columns, 16)
        out_ref[...] = turned[other % plan.turns, pl.ds(at, plan.columns), :]


def unpack_kernel(plan, *refs):
    turn_ref = refs[0]
    groups = [refs[1 + g * plan.rows : 1 + (g + 1) * plan.rows] for g in range(len(OUTBOUND))]
    out_ref, wide, gathered = refs[-3:]
    me = row_index(plan)
    fields = plan.fields
    for group, pieces in zip(OUTBOUND, groups):
        for step, piece in zip(plan.order, pieces):
            for item, field in enumerate(group):
                gathered[field, me ^ step] = piece[:, item * plan.modes : (item + 1) * plan.modes]
    for field in range(fields):
        for block in range(plan.columns // plan.group):
            rows = gathered[field, :, block * plan.group : (block + 1) * plan.group, :]
            rows = rows.reshape(256, plan.modes)
            result = matmul(rows, turn_ref[...], ((0,), (0,)))
            for side in range(2):
                wide[2 * block + side, pl.ds(field, plan.modes, stride=fields), :] = result[
                    :, side * 128 : (side + 1) * 128
                ]
    for k in range(plan.modes):
        for tile in range(plan.columns * Y // 128):
            out_ref[k, :, tile * 128 : (tile + 1) * 128] = wide[
                tile, pl.ds(k * fields, fields), :
            ].astype(BF16)


def call_plain(kernel, outs, scratch, flops, moved, *args):
    space = pl.BlockSpec(memory_space=pltpu.VMEM)
    single = not isinstance(outs, (list, tuple))
    return pl.pallas_call(
        kernel,
        out_shape=outs,
        in_specs=[space] * len(args),
        out_specs=space if single else [space] * len(outs),
        scratch_shapes=scratch,
        cost_estimate=pl.CostEstimate(flops=flops, bytes_accessed=moved, transcendentals=0),
        compiler_params=pltpu.CompilerParams(vmem_limit_bytes=KERNEL_VMEM),
    )(*args)


def tables(plan):
    z, k = np.arange(MZ), np.arange(NZ)
    cosines = np.cos(np.pi * (k[:, None] * (2 * z[None, :] + 1) % (4 * MZ)) / (2 * MZ))
    cosines = cosines.reshape(plan.turns, plan.cores, plan.modes, MZ).swapaxes(0, 1)
    cosines = cosines.reshape(plan.cores, plan.depth, MZ).astype(np.float32)
    points = np.arange(NX)
    phases = 2.0 * np.pi * (points[:, None] * points[None, :] % NX) / NX
    hartley = ((np.cos(phases) + np.sin(phases)) / math.sqrt(NX)).astype(np.float32)
    turn = np.zeros((Y, plan.group, plan.group, Y), np.float32)
    for y in range(Y):
        for m in range(plan.group):
            turn[y, m, m, y] = 1.0
    return (
        jnp.asarray((cosines * np.float32(math.sqrt(2.0 / NZ))).astype(BF16)),
        jnp.asarray((cosines * np.float32(math.sqrt(2.0 / MZ))).astype(BF16)),
        jnp.asarray(hartley.astype(BF16)),
        jnp.asarray(turn.reshape(256, 256).astype(BF16)),
    )


def exchange(plan, pieces):
    return [
        lax.ppermute(piece, ("kx", "cz"), plan.across(step)) if step else piece
        for step, piece in zip(plan.order, pieces)
    ]


def row_on_device(plan, field_modes, cotangent):
    synthesis, projection, hartley, turn = tables(plan)
    shape = jax.ShapeDtypeStruct
    local = field_modes.size
    arrived = []
    for items in INBOUND:
        width = len(items) * plan.modes
        pieces = call_plain(
            functools.partial(pack_kernel, plan, items),
            [shape((plan.columns, width), BF16)] * plan.rows,
            [
                pltpu.VMEM((plan.columns * Y // 128, plan.fields * plan.modes, 128), F32),
                pltpu.VMEM((plan.rows, plan.columns, width), BF16),
            ],
            2 * 256 * local // plan.fields * len(items),
            4 * local,
            field_modes,
            cotangent,
            turn,
        )
        arrived.append(exchange(plan, pieces))

    def swap(value):
        return lax.ppermute(value, ("kx", "cz"), plan.core_swap())

    returned = []
    kept = None
    for number, (items, outputs) in enumerate(zip(INBOUND, OUTBOUND)):
        count = len(items)
        width = count * plan.modes
        wide = count * plan.depth
        own, send = call_plain(
            functools.partial(hartley_kernel, plan, count),
            [shape((plan.points, wide), BF16)] * 2,
            [pltpu.VMEM((plan.turns, NX, width), BF16)],
            2 * NX * NX * plan.turns * width,
            4 * NX * plan.turns * width,
            hartley,
            *arrived[number],
        )
        recv = swap(send)
        out_wide = len(outputs) * plan.depth
        outs = [shape((plan.points, out_wide), BF16)] * 2
        flops = 2 * plan.points * NZ * MZ * (count + len(outputs))
        if number == 0:
            own, send, kept = call_plain(
                functools.partial(first_kernel, plan),
                outs + [shape((count, plan.points, MZ), F32)],
                [],
                flops,
                4 * count * plan.points * MZ,
                synthesis,
                projection,
                own,
                recv,
            )
        else:
            own, send = call_plain(
                functools.partial(second_kernel, plan),
                outs,
                [],
                flops,
                4 * count * plan.points * MZ,
                synthesis,
                projection,
                own,
                recv,
                kept,
            )
        recv = swap(send)
        pieces = call_plain(
            functools.partial(inverse_kernel, plan, len(outputs)),
            [shape((plan.columns, len(outputs) * plan.modes), BF16)] * plan.rows,
            [pltpu.VMEM((plan.turns, NX, len(outputs) * plan.modes), BF16)],
            2 * NX * NX * out_wide,
            4 * NX * out_wide,
            hartley,
            own,
            recv,
        )
        returned += exchange(plan, pieces)
    return call_plain(
        functools.partial(unpack_kernel, plan),
        shape(field_modes.shape, BF16),
        [
            pltpu.VMEM((plan.columns * Y // 128, plan.fields * plan.modes, 128), F32),
            pltpu.VMEM((plan.fields, plan.rows, plan.columns, plan.modes), BF16),
        ],
        2 * 256 * local,
        4 * local,
        turn,
        *returned,
    )


def on_device(kx_size, cz_size, field_modes, cotangent):
    plan = Plan(kx_size, cz_size, field_modes.shape)
    if plan.fits:
        return row_on_device(plan, field_modes, cotangent)
    return general_on_device(field_modes, cotangent)


def solution(mesh):
    return jax.shard_map(
        functools.partial(on_device, mesh.shape["kx"], mesh.shape["cz"]),
        mesh=mesh,
        in_specs=(P("cz", None, "kx"), P("cz", None, "kx")),
        out_specs=P("cz", None, "kx"),
        check_vma=False,
    )
```
